32 devices in a mesh: lb: 4 (over z), rb: 4 (over y, x), wa: 2 (over core).
Axes of the slice: x: 2, y: 2, z: 4, core: 2. Of those that a mesh axis runs over, the one named last changes fastest.
Arguments:
- initial_guess: bfloat16 [8192, 4, 128], P(('lb', 'rb')), may hold values from -6 to 6
- left_environment: bfloat16 [8, 4, 4, 512, 8192], P('wa', None, 'rb', None, 'lb'), may hold values from -12 to 12, as said below
- right_environment: bfloat16 [128, 8, 128], replicated, may hold values from -12 to 12, as said below
- operator_blocks: float32 [16, 4, 4], replicated, may hold values from -4 to 4
- operator_pairs: int32 [16, 2], replicated, may hold values from 0 to 7
Outputs:
- ritz_vector: float32 [8192, 4, 128], P(('lb', 'rb'))
- residual: float32 [8192, 4, 128], P(('lb', 'rb'))
The draws below stay inside these ranges and needn't reach their ends.
Inputs may be any that keep to these rules, and one draw needn't show every extreme that they name: `operator_pairs`: each row names the left and the right MPO index of one operator block; blocks with the same pair add. `left_environment`: for each MPO index the [8192, 8192] matrix is symmetric. `right_environment`: for each MPO index the matrix over the two right bond states is symmetric.
All inputs are finite; a program needn't handle non-finite values.
Results may differ from the reference program's by a relative error of at most 0.014.
Values may be sent and summed in bfloat16 or wider, within the bound.
A program may use at most 192 MiB of HBM per device.

```python
import jax
import jax.numpy as jnp
from jax import lax

DL = 8192
RB = 128
W = 8
NB = 16
ITERS = 3
SWEEPS = 8
S = 4
N_LB = 4
N_RB = 4


def draw_left_environment(key, part):
    noise_key = jax.random.fold_in(key, 11)
    scale_key = jax.random.fold_in(key, 12)
    noise = jax.random.normal(noise_key, (W, DL, DL), jnp.float32)
    symmetric = (noise + jnp.swapaxes(noise, 1, 2)) * (0.5 / jnp.sqrt(DL * 1.0))
    scales = jnp.exp(jax.random.uniform(scale_key, (W, DL), jnp.float32, 0.0, 2.0))
    positions = jnp.arange(DL, dtype=jnp.int32)
    symmetric = symmetric.at[:, positions, positions].add(scales)
    return symmetric.reshape(W, N_LB, N_RB, DL // (N_LB * N_RB), DL).astype(jnp.bfloat16)


def draw_right_environment(key, part):
    noise_key = jax.random.fold_in(key, 21)
    scale_key = jax.random.fold_in(key, 22)
    noise = jax.random.normal(noise_key, (RB, W, RB), jnp.float32)
    symmetric = (noise + jnp.transpose(noise, (2, 1, 0))) * (0.5 / jnp.sqrt(RB * 1.0))
    scales = jnp.exp(jax.random.uniform(scale_key, (W, RB), jnp.float32, 0.0, 2.0))
    symmetric = symmetric + jnp.eye(RB, dtype=jnp.float32)[:, None, :] * scales[None, :, :]
    return symmetric.astype(jnp.bfloat16)


def place_ends(entries, rng, least, top_value):
    shape = entries.shape
    place = [jax.random.randint(jax.random.fold_in(rng, axis), (), 0, shape[axis]) for axis in range(len(shape))]
    entries = entries.at[tuple(place)].set(least)
    longest = shape.index(max(shape))
    place[longest] = (place[longest] + 1) % shape[longest]
    return entries.at[tuple(place)].set(top_value)


def block_scale(key, dims, split, smallest, high):
    loudness, own = 1.0, jax.random.fold_in(key, 6)
    for axis_at, parts in split:
        draws = jnp.exp(jax.random.uniform(jax.random.fold_in(own, axis_at), (parts,), jnp.float32, smallest / len(split), high / len(split)))
        loudness = loudness * jnp.repeat(draws, dims[axis_at] // parts).reshape([-1 if axis == axis_at else 1 for axis in range(len(dims))])
    return loudness


def scatter_about(key, extent, deviation, reach, shards=(), kind=jnp.bfloat16):
    values = deviation * jax.random.normal(key, extent, jnp.float32)
    if shards:
        values = values * block_scale(key, extent, shards, -0.22, 0.18)
    return jnp.clip(values, -reach, reach).astype(kind)


def setup_inputs(seed: int = 0) -> dict:
    key_list = jax.random.split(jax.random.key(seed), 6)
    initial_guess = scatter_about(key_list[0], (DL, S, RB), 1.0, 6.0, ((0, 16),))
    left_environment = draw_left_environment(jax.random.fold_in(key_list[5], 71), 0)
    right_environment = draw_right_environment(jax.random.fold_in(key_list[5], 71), 0)
    operator_blocks = scatter_about(key_list[3], (NB, S, S), 0.3, 4.0, (), jnp.float32)
    operator_pairs = place_ends(jax.random.randint(key_list[4], (NB, 2), 0, W), jax.random.fold_in(key_list[4], 1), 0, W - 1).astype(jnp.int32)
    return dict(initial_guess=initial_guess, left_environment=left_environment, right_environment=right_environment, operator_blocks=operator_blocks, operator_pairs=operator_pairs)


highest = lax.Precision.HIGHEST
epsilon = 1e-06

def lowest_pair(matrix):
    matrix_order = matrix.shape[0]
    vectors = jnp.eye(matrix_order, dtype=jnp.float32)
    for rounds in range(SWEEPS):
        for first_row in range(matrix_order):
            for second_row in range(first_row + 1, matrix_order):
                rotation_angle = 0.5 * jnp.arctan2(2.0 * matrix[first_row, second_row], matrix[second_row, second_row] - matrix[first_row, first_row])
                cosine = jnp.cos(rotation_angle)
                sine_value = jnp.sin(rotation_angle)
                rotation = jnp.eye(matrix_order, dtype=jnp.float32)
                rotation = rotation.at[first_row, first_row].set(cosine).at[second_row, second_row].set(cosine)
                rotation = rotation.at[first_row, second_row].set(sine_value).at[second_row, first_row].set(-sine_value)
                matrix = jnp.dot(rotation.T, jnp.dot(matrix, rotation, precision=highest), precision=highest)
                vectors = jnp.dot(vectors, rotation, precision=highest)
    values = jnp.diagonal(matrix)
    chosen = (jnp.arange(matrix_order, dtype=jnp.int32) == jnp.argmin(values).astype(jnp.int32)).astype(jnp.float32)
    ritz_value = jnp.sum(values * chosen)
    weights = jnp.dot(vectors, chosen, precision=highest)
    weights = jnp.where(weights[0] < 0.0, -weights, weights)
    return (ritz_value, weights)

def dense_operator(operator_blocks, operator_pairs, levels):
    symmetric = 0.5 * (operator_blocks + jnp.swapaxes(operator_blocks, 1, 2))
    indices = jnp.arange(levels, dtype=jnp.int32)
    left_hot = (operator_pairs[:, 0:1] == indices[None, :]).astype(jnp.float32)
    right_hot = (operator_pairs[:, 1:2] == indices[None, :]).astype(jnp.float32)
    return jnp.einsum('nw,nv,nts->wvts', left_hot, right_hot, symmetric, precision=highest)

def contract_right(vector_rows, right_matrix, local_operator):
    row_count, physical, window = vector_rows.shape
    levels = local_operator.shape[1]
    mixed = jnp.dot(vector_rows.reshape(row_count * physical, window), right_matrix, preferred_element_type=jnp.float32)
    mixed = mixed.reshape(row_count, physical, levels, window)
    return jnp.einsum('kvts,nsvb->kntb', local_operator, mixed, precision=highest).astype(jnp.bfloat16)

def combine(members, weights):
    total = weights[0] * members[0]
    for member_index in range(1, len(members)):
        total = total + weights[member_index] * members[member_index]
    return total

def reference(initial_guess, left_environment, right_environment, operator_blocks, operator_pairs):
    total_count = DL * S * RB
    left_matrix = left_environment.reshape(W, DL, DL)
    right_matrix = right_environment.reshape(RB, W * RB)
    operator = dense_operator(operator_blocks, operator_pairs, W)

    def apply_hamiltonian(vector):
        inner_terms = contract_right(vector.astype(jnp.bfloat16), right_matrix, operator)
        flat = inner_terms.reshape(W, DL, S * RB)
        image = jnp.zeros((DL, S * RB), jnp.float32)
        for level in range(W):
            image = image + jnp.dot(left_matrix[level], flat[level], preferred_element_type=jnp.float32)
        return image.reshape(DL, S, RB)

    def mean_product(first_array, second_array):
        return jnp.sum(first_array * second_array) / total_count
    left_diag = jnp.diagonal(left_matrix, axis1=1, axis2=2).astype(jnp.float32)
    operator_diag = jnp.diagonal(operator, axis1=2, axis2=3)
    right_diag = jnp.diagonal(right_environment, axis1=0, axis2=2).astype(jnp.float32)
    diagonal_values = jnp.einsum('ka,kvs,vb->asb', left_diag, operator_diag, right_diag, precision=highest)
    start_vector = initial_guess.astype(jnp.float32)
    basis = [start_vector * lax.rsqrt(mean_product(start_vector, start_vector) + epsilon)]
    images = [apply_hamiltonian(basis[0])]
    subspace = jnp.zeros((ITERS + 1, ITERS + 1), jnp.float32)
    subspace = subspace.at[0, 0].set(mean_product(basis[0], images[0]))
    for step_index in range(ITERS):
        filled = step_index + 1
        ritz_value, weights = lowest_pair(subspace[:filled, :filled])
        ritz_now = combine(basis, weights)
        residual_now = combine(images, weights) - ritz_value * ritz_now
        correction = residual_now / (jnp.abs(diagonal_values - ritz_value) + 1.0)
        correlations = jnp.stack([mean_product(member, correction) for member in basis])
        correction = correction - combine(basis, correlations)
        new_vector = correction * lax.rsqrt(mean_product(correction, correction) + epsilon)
        new_image = apply_hamiltonian(new_vector)
        basis.append(new_vector)
        images.append(new_image)
        row_values = jnp.stack([mean_product(member, new_image) for member in basis])
        subspace = subspace.at[filled, :filled + 1].set(row_values).at[:filled + 1, filled].set(row_values)
    ritz_value, weights = lowest_pair(subspace)
    ritz_vector = combine(basis, weights)
    residual = combine(images, weights) - ritz_value * ritz_vector
    return (ritz_vector, residual)
```

```python
import functools

import jax
import jax.numpy as jnp
from jax import lax
from jax.experimental import pallas as pl
from jax.experimental.pallas import tpu as pltpu
from jax.sharding import PartitionSpec as P

ITERS = 3
SWEEPS = 8

highest = lax.Precision.HIGHEST
epsilon = 1e-06

TILE = (8, 128)
LANES = 128
VMEM_BYTES = 66_000_000
MESH_IDS = pl.DeviceIdType.MESH


def half_angle(y, x):
    scale = jnp.maximum(jnp.abs(x), jnp.abs(y))
    zero = scale == 0.0
    inverse = 1.0 / jnp.where(zero, 1.0, scale)
    xs, ys = x * inverse, y * inverse
    h = jnp.sqrt(xs * xs + ys * ys)
    h = jnp.where(zero, 1.0, h)
    big = jnp.sqrt(0.5 * (1.0 + jnp.abs(xs) / h))
    small = 0.5 * jnp.abs(ys) / (h * big)
    positive = x >= 0.0
    cosine = jnp.where(positive, big, small)
    sine = jnp.where(positive, small, big) * jnp.where(y < 0.0, -1.0, 1.0)
    return jnp.where(zero, 1.0, cosine), jnp.where(zero, 0.0, sine)


def lowest_pair(order, entry):
    def at(i, j):
        return (min(i, j), max(i, j))

    one, none = jnp.full(TILE, 1.0, jnp.float32), jnp.full(TILE, 0.0, jnp.float32)
    if order == 1:
        return entry(0, 0), [one]
    keys = [(i, j) for i in range(order) for j in range(i, order)]
    start = tuple(entry(i, j) for i, j in keys)
    vectors0 = tuple(one if i == j else none for i in range(order) for j in range(order))

    def sweep(_, carry):
        m = dict(zip(keys, carry[0]))
        v = list(carry[1])
        for p in range(order):
            for q in range(p + 1, order):
                a, b, d = m[(p, p)], m[(p, q)], m[(q, q)]
                c, s = half_angle(2.0 * b, d - a)
                m[(p, p)] = c * (c * a - s * b) - s * (c * b - s * d)
                m[(p, q)] = s * (c * a - s * b) + c * (c * b - s * d)
                m[(q, q)] = s * (s * a + c * b) + c * (s * b + c * d)
                for i in range(order):
                    if i != p and i != q:
                        x, y = m[at(i, p)], m[at(i, q)]
                        m[at(i, p)] = c * x - s * y
                        m[at(i, q)] = s * x + c * y
                    x, y = v[i * order + p], v[i * order + q]
                    v[i * order + p] = c * x - s * y
                    v[i * order + q] = s * x + c * y
        return tuple(m[key] for key in keys), tuple(v)

    values, vectors = lax.fori_loop(0, SWEEPS, sweep, (start, vectors0))
    m = dict(zip(keys, values))
    best = m[(0, 0)]
    weights = [vectors[i * order] for i in range(order)]
    for j in range(1, order):
        better = m[(j, j)] < best
        best = jnp.where(better, m[(j, j)], best)
        weights = [
            jnp.where(better, vectors[i * order + j], weights[i]) for i in range(order)
        ]
    sign = jnp.where(weights[0] < 0.0, -1.0, 1.0)
    return best, [weight * sign for weight in weights]


def dense_operator(operator_blocks, operator_pairs, levels):
    symmetric = 0.5 * (operator_blocks + jnp.swapaxes(operator_blocks, 1, 2))
    indices = jnp.arange(levels, dtype=jnp.int32)
    left_hot = (operator_pairs[:, 0:1] == indices[None, :]).astype(jnp.float32)
    right_hot = (operator_pairs[:, 1:2] == indices[None, :]).astype(jnp.float32)
    return jnp.einsum("nw,nv,nts->wvts", left_hot, right_hot, symmetric, precision=highest)


def fold(block):
    rows, columns = block.shape
    total = None
    for r in range(0, rows, TILE[0]):
        for c in range(0, columns, LANES):
            piece = block[r : r + TILE[0], c : c + LANES]
            total = piece if total is None else total + piece
    return total


def scalar_of(tile):
    return tile[0:1, 0:1]


def davidson_kernel(
    dims,
    op_ref, guess_ref, right_ref, left_hbm,
    vec_out, res_out,
    left, joint, xall, inner, wsend, wrecv, zsend, zrecv,
    basis, images, diag, vec, img, rows_ref, dots, sub, pair,
    load_sem, gx_send, gx_recv, gw_send, gw_recv, w_send, w_recv, z_send, z_recv,
    d_sem, dot_send, dot_recv, out_sem,
):
    (n_lb, n_rb, n_wa, rb_minor, own_rows, half, width, window, physical, levels,
     local_levels, total_count) = dims
    devices = n_lb * n_rb * n_wa
    i, j, w = lax.axis_index("lb"), lax.axis_index("rb"), lax.axis_index("wa")
    me = (i * n_rb + j) * n_wa + w
    other = 1 - w
    partner = (i, j, other)
    chunk = min(32, half)
    rb_major = n_rb // rb_minor

    def device_of(flat):
        return (
            lax.div(flat, n_rb * n_wa),
            lax.rem(lax.div(flat, n_wa), n_rb),
            lax.rem(flat, n_wa),
        )

    def rb_step(step, sign):
        high, low = lax.div(j, rb_minor), lax.rem(j, rb_minor)
        dh, dl = lax.div(step, rb_minor), lax.rem(step, rb_minor)
        if sign > 0:
            high, low = lax.rem(high + dh, rb_major), lax.rem(low + dl, rb_minor)
        else:
            high = lax.rem(high - dh + rb_major, rb_major)
            low = lax.rem(low - dl + rb_minor, rb_minor)
        return high * rb_minor + low

    def remote(src, dst, send, recv, target):
        return pltpu.make_async_remote_copy(
            src_ref=src, dst_ref=dst, send_sem=send, recv_sem=recv,
            device_id=target, device_id_type=MESH_IDS,
        )

    def rows_at(index, size=chunk):
        return pl.ds(pl.multiple_of(index, size), size)

    def over_chunks(body, init):
        return lax.fori_loop(0, half // chunk, body, init)

    barrier = pltpu.get_barrier_semaphore()

    def greet(step, carry):
        target = device_of(lax.rem(me + step, devices))
        pl.semaphore_signal(barrier, inc=1, device_id=target, device_id_type=MESH_IDS)
        return carry

    lax.fori_loop(1, devices, greet, 0)

    def target_block(t):
        return lax.rem(i + 1 + t, n_lb)

    def load_block(t):
        span = pl.ds(pl.multiple_of(target_block(t) * own_rows, own_rows), own_rows)
        return pltpu.make_async_copy(
            left_hbm.at[:, span, :], left.at[:, span, :], load_sem.at[t]
        )

    for t in range(n_lb):
        load_block(t).start()

    xall[j, w] = guess_ref[...]

    def prepare(c, carry):
        at = rows_at(c * chunk)
        vec[at, :] = guess_ref[at, :].astype(jnp.float32)
        zeros = jnp.zeros((chunk, width), jnp.float32)
        for n in range(ITERS):
            basis[n, at, :] = zeros
            images[n, at, :] = zeros
        return carry

    over_chunks(prepare, 0)
    pl.semaphore_wait(barrier, devices - 1)

    def gather_rb(step):
        q = rb_step(step, 1)
        return remote(
            xall.at[j, w], xall.at[j, w], gx_send.at[step], gx_recv.at[step], (i, q, w)
        )

    def gather_wa(step):
        q = rb_step(step, -1)
        return remote(xall.at[q, w], xall.at[q, w], gw_send.at[step], gw_recv.at[step], partner)

    def send_vector():
        gather_wa(0).start()
        for step in range(1, n_rb):
            gather_rb(step).start()

    send_vector()

    op_base = w * (local_levels * levels * physical * physical)
    band = min(32, window)

    def make_joint(index, carry):
        k = lax.div(index, window // band)
        r0 = lax.rem(index, window // band) * band
        mats = [right_ref[v, pl.ds(pl.multiple_of(r0, band), band), :] for v in range(levels)]
        for s in range(physical):
            for t in range(physical):
                total = None
                for v in range(levels):
                    at = op_base + ((k * levels + v) * physical + t) * physical + s
                    term = op_ref[at] * mats[v]
                    total = term if total is None else total + term
                high = total.astype(jnp.bfloat16)
                low = (total - high.astype(jnp.float32)).astype(jnp.bfloat16)
                rows = pl.ds(pl.multiple_of(s * window + r0, band), band)
                joint[k, 0, rows, t * window : (t + 1) * window] = high
                joint[k, 1, rows, t * window : (t + 1) * window] = low
        return carry

    lax.fori_loop(0, local_levels * (window // band), make_joint, 0)

    eye = lax.broadcasted_iota(jnp.int32, (window, window), 0) == lax.broadcasted_iota(
        jnp.int32, (window, window), 1
    )
    right_diag = [
        jnp.sum(jnp.where(eye, right_ref[v], 0.0), axis=0, keepdims=True) for v in range(levels)
    ]
    for k in range(local_levels):
        for s in range(physical):
            total = None
            for v in range(levels):
                at = op_base + ((k * levels + v) * physical + s) * physical + s
                term = op_ref[at] * right_diag[v]
                total = term if total is None else total + term
            rows_ref[k, :, s * window : (s + 1) * window] = total

    def diagonal_part(r0):
        first = j * own_rows + r0
        base = lax.div(first, LANES) * LANES
        shift = first - base
        lane = lax.broadcasted_iota(jnp.int32, (chunk, LANES), 1)
        row = lax.broadcasted_iota(jnp.int32, (chunk, LANES), 0)
        mask = lane == row + shift
        total = None
        for k in range(local_levels):
            block = left[
                k,
                pl.ds(pl.multiple_of(i * own_rows + r0, chunk), chunk),
                pl.ds(pl.multiple_of(base, LANES), LANES),
            ].astype(jnp.float32)
            column = jnp.sum(jnp.where(mask, block, 0.0), axis=1, keepdims=True)
            term = column * rows_ref[k]
            total = term if total is None else total + term
        return total

    def all_reduce(slot, tiles):
        rows = [jnp.sum(tile, axis=0, keepdims=True) for tile in tiles]
        lane8 = lax.broadcasted_iota(jnp.int32, TILE, 1)
        row8 = lax.broadcasted_iota(jnp.int32, TILE, 0)
        stacked = jnp.zeros(TILE, jnp.float32)
        for n, row in enumerate(rows):
            stacked = jnp.where(row8 == n, row, stacked)
        column = jnp.sum(stacked, axis=1, keepdims=True)
        line = jnp.sum(jnp.where(lane8 == row8, column, 0.0), axis=0, keepdims=True)
        dots[slot, me] = line

        def send(step, carry):
            target = device_of(lax.rem(me + step, devices))
            remote(
                dots.at[slot, me], dots.at[slot, me], dot_send.at[slot], dot_recv.at[slot], target
            ).start()
            return carry

        lax.fori_loop(1, devices, send, 0)
        most = dots.at[slot, pl.ds(0, devices - 1)]
        pltpu.make_async_copy(most, most, dot_send.at[slot]).wait()
        pltpu.make_async_copy(most, most, dot_recv.at[slot]).wait()
        total = jnp.sum(dots[slot], axis=0)
        spread = jnp.sum(jnp.where(lane8 == row8, total, 0.0), axis=1, keepdims=True)
        spread = spread * (1.0 / total_count)
        return [jnp.broadcast_to(spread[n : n + 1, :], TILE) for n in range(len(tiles))]

    def inner_block(q, u):
        x = xall[q, u]
        at = pl.ds(pl.multiple_of(q * own_rows + u * half, half), half)

        def one(k, carry):
            value = jnp.dot(x, joint[k, 0], preferred_element_type=jnp.float32)
            value = value + jnp.dot(x, joint[k, 1], preferred_element_type=jnp.float32)
            inner[k, at, :] = value.astype(jnp.bfloat16)
            return carry

        lax.fori_loop(0, local_levels, one, 0)

    def rows_times(block, u):
        at = pl.ds(pl.multiple_of(block * own_rows + u * half, half), half)
        total = None
        for k in range(local_levels):
            term = jnp.dot(left[k, at, :], inner[k], preferred_element_type=jnp.float32)
            total = term if total is None else total + term
        return total

    def exchange(t):
        return remote(wsend.at[t], wrecv.at[t], w_send.at[t], w_recv.at[t], partner)

    def scatter(t):
        return remote(
            zsend.at[t], zrecv.at[t], z_send.at[t], z_recv.at[t], (target_block(t), j, w)
        )

    def iteration(it, carry):
        inner_block(j, w)
        gather_wa(0).wait_recv()
        inner_block(j, other)

        def arrive(step, c):
            q = rb_step(step, -1)
            gather_rb(step).wait_recv()
            gather_wa(step).start()
            inner_block(q, w)
            gather_wa(step).wait_recv()
            inner_block(q, other)
            return c

        lax.fori_loop(1, n_rb, arrive, 0)

        def block_sum(t):
            block = target_block(t)

            @pl.when(it == 0)
            def _():
                load_block(t).wait()

            wsend[t] = rows_times(block, other)
            exchange(t).start()
            value = rows_times(block, w)
            exchange(t).wait_recv()
            return value + wrecv[t]

        def away(t, c):
            zsend[t] = block_sum(t).astype(jnp.bfloat16)
            scatter(t).start()
            return c

        lax.fori_loop(0, n_lb - 1, away, 0)
        img[...] = block_sum(n_lb - 1)

        @pl.when(it == 0)
        def _():
            def mine(c, carry):
                diag[rows_at(c * chunk), :] = diagonal_part(w * half + c * chunk)
                return carry

            def theirs(c, carry):
                images[ITERS, rows_at(c * chunk), :] = diagonal_part(other * half + c * chunk)
                return carry

            over_chunks(theirs, 0)
            swap = remote(images.at[ITERS], basis.at[ITERS], d_sem.at[0], d_sem.at[1], partner)
            swap.start()
            over_chunks(mine, 0)
            swap.wait()

            def join(c, carry):
                at = rows_at(c * chunk)
                diag[at, :] = diag[at, :] + basis[ITERS, at, :]
                return carry

            over_chunks(join, 0)

        gather_wa(0).wait_send()
        for step in range(1, n_rb):
            gather_rb(step).wait_send()
            gather_wa(step).wait_send()
        for t in range(n_lb):
            exchange(t).wait_send()
        for t in range(n_lb - 1):
            scatter(t).wait_send()
        for t in range(n_lb - 1):
            scatter(t).wait_recv()

        def measure(c, sums):
            at = rows_at(c * chunk)
            y = img[at, :]
            for t in range(n_lb - 1):
                y = y + zrecv[t, at, :].astype(jnp.float32)
            img[at, :] = y
            x = vec[at, :]
            parts = [x * x, x * y] + [basis[n, at, :] * y for n in range(ITERS)]
            return tuple(total + fold(part) for total, part in zip(sums, parts))

        zero = jnp.zeros(TILE, jnp.float32)
        sums = over_chunks(measure, (zero,) * (2 + ITERS))
        sums = all_reduce(1, sums)
        scale = lax.rsqrt(sums[0] + epsilon)

        def keep(c, carry):
            at = rows_at(c * chunk)
            basis[it, at, :] = vec[at, :] * scalar_of(scale)
            images[it, at, :] = img[at, :] * scalar_of(scale)
            return carry

        over_chunks(keep, 0)

        for order in range(1, ITERS + 2):

            @pl.when(it == order - 1)
            def _():
                last = order - 1
                for n in range(last):
                    sub[n * (ITERS + 1) + last] = sums[2 + n] * scale
                sub[last * (ITERS + 1) + last] = sums[1] * scale * scale
                value, weights = lowest_pair(order, lambda a, b: sub[a * (ITERS + 1) + b])
                pair[0] = value
                for n in range(ITERS + 1):
                    pair[n + 1] = weights[n] if n < order else zero

        def ritz(at, members):
            value = scalar_of(pair[0])
            weight = [scalar_of(pair[n + 1]) for n in range(members)]
            u = weight[0] * basis[0, at, :]
            r = weight[0] * images[0, at, :]
            for n in range(1, members):
                u = u + weight[n] * basis[n, at, :]
                r = r + weight[n] * images[n, at, :]
            return value, u, r - value * u

        @pl.when(it < ITERS)
        def _():
            def correct(c, sums):
                at = rows_at(c * chunk)
                value, _, r = ritz(at, ITERS)
                x = r / (jnp.abs(diag[at, :] - value) + 1.0)
                vec[at, :] = x
                return tuple(
                    total + fold(basis[n, at, :] * x) for n, total in enumerate(sums)
                )

            overlaps = all_reduce(0, over_chunks(correct, (zero,) * ITERS))

            def project(c, carry):
                at = rows_at(c * chunk)
                x = vec[at, :]
                total = scalar_of(overlaps[0]) * basis[0, at, :]
                for n in range(1, ITERS):
                    total = total + scalar_of(overlaps[n]) * basis[n, at, :]
                x = x - total
                vec[at, :] = x
                xall[j, w, at, :] = x.astype(jnp.bfloat16)
                return carry

            over_chunks(project, 0)
            send_vector()

        @pl.when(it == ITERS)
        def _():
            def finish(c, carry):
                at = rows_at(c * chunk)
                _, u, r = ritz(at, ITERS + 1)
                vec[at, :] = u
                img[at, :] = r
                return carry

            over_chunks(finish, 0)
            span = pl.ds(pl.multiple_of(w * half, half), half)
            moves = []
            for n, (src, dst) in enumerate(((vec, vec_out), (img, res_out))):
                moves.append(
                    remote(src, dst.at[span, :], out_sem.at[3 * n], out_sem.at[3 * n + 1], partner)
                )
                moves.append(pltpu.make_async_copy(src, dst.at[span, :], out_sem.at[3 * n + 2]))
            for move in moves:
                move.start()
            for move in moves:
                move.wait()

        return carry

    lax.fori_loop(0, ITERS + 1, iteration, 0)


def minor_of(size):
    best = 1
    for candidate in range(1, size + 1):
        if candidate * candidate <= size and size % candidate == 0:
            best = candidate
    return best


def per_device(initial_guess, left_environment, right_environment, operator_blocks, operator_pairs):
    own_rows, physical, window = initial_guess.shape
    width = physical * window
    levels = right_environment.shape[1]
    local_levels, coarse = left_environment.shape[:2]
    contracted = left_environment.shape[4]
    n_lb, n_rb, n_wa = lax.axis_size("lb"), lax.axis_size("rb"), lax.axis_size("wa")
    half = own_rows // n_wa
    total_count = own_rows * physical * window * n_lb * n_rb
    devices = n_lb * n_rb * n_wa

    operator = dense_operator(operator_blocks, operator_pairs, levels).reshape(-1)
    right = jnp.transpose(right_environment, (1, 0, 2)).astype(jnp.float32)
    left_matrix = left_environment.reshape(local_levels, coarse * own_rows, contracted)
    guess = lax.dynamic_slice_in_dim(initial_guess, lax.axis_index("wa") * half, half, 0)
    guess = guess.reshape(half, width)

    dims = (n_lb, n_rb, n_wa, minor_of(n_rb), own_rows, half, width, window, physical, levels,
            local_levels, total_count)
    f32, bf16 = jnp.float32, jnp.bfloat16
    members = ITERS + 1
    dma = pltpu.SemaphoreType.DMA
    outs = jax.ShapeDtypeStruct((own_rows, width), f32)
    vmem = pl.BlockSpec(memory_space=pltpu.VMEM)
    hbm = pl.BlockSpec(memory_space=pl.ANY)
    vectors, residuals = pl.pallas_call(
        functools.partial(davidson_kernel, dims),
        out_shape=(outs, outs),
        in_specs=[pl.BlockSpec(memory_space=pltpu.SMEM), vmem, vmem, hbm],
        out_specs=(hbm, hbm),
        scratch_shapes=[
            pltpu.VMEM((local_levels, coarse * own_rows, contracted), bf16),
            pltpu.VMEM((local_levels, 2, width, width), bf16),
            pltpu.VMEM((n_rb, n_wa, half, width), bf16),
            pltpu.VMEM((local_levels, contracted, width), bf16),
            pltpu.VMEM((n_lb, half, width), f32),
            pltpu.VMEM((n_lb, half, width), f32),
            pltpu.VMEM((n_lb - 1, half, width), bf16),
            pltpu.VMEM((n_lb - 1, half, width), bf16),
            pltpu.VMEM((members, half, width), f32),
            pltpu.VMEM((members, half, width), f32),
            pltpu.VMEM((half, width), f32),
            pltpu.VMEM((half, width), f32),
            pltpu.VMEM((half, width), f32),
            pltpu.VMEM((local_levels, 1, width), f32),
            pltpu.VMEM((2, devices, 1, LANES), f32),
            pltpu.VMEM((members * members,) + TILE, f32),
            pltpu.VMEM((members + 1,) + TILE, f32),
            dma((n_lb,)),
            dma((n_rb,)),
            dma((n_rb,)),
            dma((n_rb,)),
            dma((n_rb,)),
            dma((n_lb,)),
            dma((n_lb,)),
            dma((n_lb,)),
            dma((n_lb,)),
            dma((2,)),
            dma((2,)),
            dma((2,)),
            dma((6,)),
        ],
        compiler_params=pltpu.CompilerParams(
            collective_id=0, has_side_effects=True, vmem_limit_bytes=VMEM_BYTES
        ),
        name="davidson",
    )(operator, guess, right, left_matrix)

    shape = (own_rows, physical, window)
    return vectors.reshape(shape), residuals.reshape(shape)


def solution(mesh):
    in_specs = (P(("lb", "rb"), None, None), P("wa", None, "rb", None, "lb"), P(), P(), P())
    out_specs = (P(("lb", "rb"), None, None), P(("lb", "rb"), None, None))
    return jax.shard_map(
        per_device, mesh=mesh, in_specs=in_specs, out_specs=out_specs, check_vma=False
    )
```

```python
import functools

import jax
import jax.numpy as jnp
from jax import lax
from jax.experimental import pallas as pl
from jax.experimental.pallas import tpu as pltpu
from jax.sharding import PartitionSpec as P

ITERS = 3
SWEEPS = 8

highest = lax.Precision.HIGHEST
epsilon = 1e-06

TILE = (8, 128)
LANES = 128
VMEM_BYTES = 66_000_000
MESH_IDS = pl.DeviceIdType.MESH


def half_angle(y, x):
    scale = jnp.maximum(jnp.abs(x), jnp.abs(y))
    zero = scale == 0.0
    inverse = 1.0 / jnp.where(zero, 1.0, scale)
    xs, ys = x * inverse, y * inverse
    h = jnp.sqrt(xs * xs + ys * ys)
    h = jnp.where(zero, 1.0, h)
    big = jnp.sqrt(0.5 * (1.0 + jnp.abs(xs) / h))
    small = 0.5 * jnp.abs(ys) / (h * big)
    positive = x >= 0.0
    cosine = jnp.where(positive, big, small)
    sine = jnp.where(positive, small, big) * jnp.where(y < 0.0, -1.0, 1.0)
    return jnp.where(zero, 1.0, cosine), jnp.where(zero, 0.0, sine)


def lowest_pair(order, entry):
    def at(i, j):
        return (min(i, j), max(i, j))

    one, none = jnp.full(TILE, 1.0, jnp.float32), jnp.full(TILE, 0.0, jnp.float32)
    if order == 1:
        return entry(0, 0), [one]
    keys = [(i, j) for i in range(order) for j in range(i, order)]
    start = tuple(entry(i, j) for i, j in keys)
    vectors0 = tuple(one if i == j else none for i in range(order) for j in range(order))

    def sweep(_, carry):
        m = dict(zip(keys, carry[0]))
        v = list(carry[1])
        for p in range(order):
            for q in range(p + 1, order):
                a, b, d = m[(p, p)], m[(p, q)], m[(q, q)]
                c, s = half_angle(2.0 * b, d - a)
                m[(p, p)] = c * (c * a - s * b) - s * (c * b - s * d)
                m[(p, q)] = s * (c * a - s * b) + c * (c * b - s * d)
                m[(q, q)] = s * (s * a + c * b) + c * (s * b + c * d)
                for i in range(order):
                    if i != p and i != q:
                        x, y = m[at(i, p)], m[at(i, q)]
                        m[at(i, p)] = c * x - s * y
                        m[at(i, q)] = s * x + c * y
                    x, y = v[i * order + p], v[i * order + q]
                    v[i * order + p] = c * x - s * y
                    v[i * order + q] = s * x + c * y
        return tuple(m[key] for key in keys), tuple(v)

    values, vectors = lax.fori_loop(0, SWEEPS, sweep, (start, vectors0))
    m = dict(zip(keys, values))
    best = m[(0, 0)]
    weights = [vectors[i * order] for i in range(order)]
    for j in range(1, order):
        better = m[(j, j)] < best
        best = jnp.where(better, m[(j, j)], best)
        weights = [
            jnp.where(better, vectors[i * order + j], weights[i]) for i in range(order)
        ]
    sign = jnp.where(weights[0] < 0.0, -1.0, 1.0)
    return best, [weight * sign for weight in weights]


def dense_operator(operator_blocks, operator_pairs, levels):
    symmetric = 0.5 * (operator_blocks + jnp.swapaxes(operator_blocks, 1, 2))
    indices = jnp.arange(levels, dtype=jnp.int32)
    left_hot = (operator_pairs[:, 0:1] == indices[None, :]).astype(jnp.float32)
    right_hot = (operator_pairs[:, 1:2] == indices[None, :]).astype(jnp.float32)
    return jnp.einsum("nw,nv,nts->wvts", left_hot, right_hot, symmetric, precision=highest)


def fold(block):
    rows, columns = block.shape
    total = None
    for r in range(0, rows, TILE[0]):
        for c in range(0, columns, LANES):
            piece = block[r : r + TILE[0], c : c + LANES]
            total = piece if total is None else total + piece
    return total


def scalar_of(tile):
    return tile[0:1, 0:1]


def davidson_kernel(
    dims,
    op_ref, guess_ref, right_ref, left_hbm,
    vec_out, res_out,
    left, joint, xall, inner, wsend, wrecv, zsend, zrecv,
    basis, images, diag, vec, img, rows_ref, dots, sub, pair, over,
    load_sem, gx_send, gx_recv, gw_send, gw_recv, w_send, w_recv, z_send, z_recv,
    d_sem, dot_send, dot_recv, out_sem,
):
    (n_lb, n_rb, n_wa, rb_minor, own_rows, half, width, window, physical, levels,
     local_levels, total_count) = dims
    devices = n_lb * n_rb * n_wa
    i, j, w = lax.axis_index("lb"), lax.axis_index("rb"), lax.axis_index("wa")
    me = (i * n_rb + j) * n_wa + w
    other = 1 - w
    partner = (i, j, other)
    chunk = min(32, half)
    rb_major = n_rb // rb_minor

    def device_of(flat):
        return (
            lax.div(flat, n_rb * n_wa),
            lax.rem(lax.div(flat, n_wa), n_rb),
            lax.rem(flat, n_wa),
        )

    def rb_step(step, sign):
        high, low = lax.div(j, rb_minor), lax.rem(j, rb_minor)
        dh, dl = lax.div(step, rb_minor), lax.rem(step, rb_minor)
        if sign > 0:
            high, low = lax.rem(high + dh, rb_major), lax.rem(low + dl, rb_minor)
        else:
            high = lax.rem(high - dh + rb_major, rb_major)
            low = lax.rem(low - dl + rb_minor, rb_minor)
        return high * rb_minor + low

    def remote(src, dst, send, recv, target):
        return pltpu.make_async_remote_copy(
            src_ref=src, dst_ref=dst, send_sem=send, recv_sem=recv,
            device_id=target, device_id_type=MESH_IDS,
        )

    def rows_at(index, size=chunk):
        return pl.ds(pl.multiple_of(index, size), size)

    def over_chunks(body, init):
        return lax.fori_loop(0, half // chunk, body, init)

    barrier = pltpu.get_barrier_semaphore()

    def greet(step, carry):
        target = device_of(lax.rem(me + step, devices))
        pl.semaphore_signal(barrier, inc=1, device_id=target, device_id_type=MESH_IDS)
        return carry

    lax.fori_loop(1, devices, greet, 0)

    long_side = jnp.maximum(i, n_lb - 1 - i)
    short_side = jnp.minimum(i, n_lb - 1 - i)
    toward = jnp.where(2 * i <= n_lb - 1, 1, -1)
    interior = jnp.logical_and(i > 0, i < n_lb - 1)

    def target_block(t):
        if t == n_lb - 1:
            return i
        rest = t - (long_side - short_side)
        pair_at = jnp.maximum(rest, 0)
        near = short_side - lax.div(pair_at, 2)
        sign = jnp.where(lax.rem(pair_at, 2) == 0, -toward, toward)
        return jnp.where(rest < 0, i + toward * (long_side - t), i + sign * near)

    def load_block(t):
        span = pl.ds(pl.multiple_of(target_block(t) * own_rows, own_rows), own_rows)
        return pltpu.make_async_copy(
            left_hbm.at[:, span, :], left.at[:, span, :], load_sem.at[t]
        )

    for t in range(n_lb):
        load_block(t).start()

    xall[j, w] = guess_ref[...]

    def prepare(c, carry):
        at = rows_at(c * chunk)
        vec[at, :] = guess_ref[at, :].astype(jnp.float32)
        zeros = jnp.zeros((chunk, width), jnp.float32)
        for n in range(ITERS):
            basis[n, at, :] = zeros
            images[n, at, :] = zeros
        return carry

    over_chunks(prepare, 0)
    for n in range(ITERS):
        over[n] = jnp.zeros(TILE, jnp.float32)

    @pl.when(i == 0)
    def _():
        zrecv[i] = jnp.zeros((half, width), jnp.bfloat16)

    @pl.when(i == n_lb - 1)
    def _():
        zrecv[n_lb] = jnp.zeros((half, width), jnp.bfloat16)

    pl.semaphore_wait(barrier, devices - 1)

    def gather_rb(step):
        q = rb_step(step, 1)
        return remote(
            xall.at[j, w], xall.at[j, w], gx_send.at[step], gx_recv.at[step], (i, q, w)
        )

    def gather_wa(step):
        q = rb_step(step, -1)
        return remote(xall.at[q, w], xall.at[q, w], gw_send.at[step], gw_recv.at[step], partner)

    def send_vector():
        gather_wa(0).start()
        for step in range(1, n_rb):
            gather_rb(step).start()

    send_vector()

    op_base = w * (local_levels * levels * physical * physical)
    band = min(32, window)

    def make_joint(index, carry):
        k = lax.div(index, window // band)
        r0 = lax.rem(index, window // band) * band
        mats = [right_ref[v, pl.ds(pl.multiple_of(r0, band), band), :] for v in range(levels)]
        for s in range(physical):
            for t in range(physical):
                total = None
                for v in range(levels):
                    at = op_base + ((k * levels + v) * physical + t) * physical + s
                    term = op_ref[at] * mats[v]
                    total = term if total is None else total + term
                high = total.astype(jnp.bfloat16)
                low = (total - high.astype(jnp.float32)).astype(jnp.bfloat16)
                rows = pl.ds(pl.multiple_of(s * window + r0, band), band)
                joint[k, 0, rows, t * window : (t + 1) * window] = high
                joint[k, 1, rows, t * window : (t + 1) * window] = low
        return carry

    lax.fori_loop(0, local_levels * (window // band), make_joint, 0)

    eye = lax.broadcasted_iota(jnp.int32, (window, window), 0) == lax.broadcasted_iota(
        jnp.int32, (window, window), 1
    )
    right_diag = [
        jnp.sum(jnp.where(eye, right_ref[v], 0.0), axis=0, keepdims=True) for v in range(levels)
    ]
    for k in range(local_levels):
        for s in range(physical):
            total = None
            for v in range(levels):
                at = op_base + ((k * levels + v) * physical + s) * physical + s
                term = op_ref[at] * right_diag[v]
                total = term if total is None else total + term
            rows_ref[k, :, s * window : (s + 1) * window] = total

    def diagonal_part(r0):
        first = j * own_rows + r0
        base = lax.div(first, LANES) * LANES
        shift = first - base
        lane = lax.broadcasted_iota(jnp.int32, (chunk, LANES), 1)
        row = lax.broadcasted_iota(jnp.int32, (chunk, LANES), 0)
        mask = lane == row + shift
        total = None
        for k in range(local_levels):
            block = left[
                k,
                pl.ds(pl.multiple_of(i * own_rows + r0, chunk), chunk),
                pl.ds(pl.multiple_of(base, LANES), LANES),
            ].astype(jnp.float32)
            column = jnp.sum(jnp.where(mask, block, 0.0), axis=1, keepdims=True)
            term = column * rows_ref[k]
            total = term if total is None else total + term
        return total

    lane8 = lax.broadcasted_iota(jnp.int32, TILE, 1)
    row8 = lax.broadcasted_iota(jnp.int32, TILE, 0)

    def reduce_start(slot, tiles):
        rows = [jnp.sum(tile, axis=0, keepdims=True) for tile in tiles]
        stacked = jnp.zeros(TILE, jnp.float32)
        for n, row in enumerate(rows):
            stacked = jnp.where(row8 == n, row, stacked)
        column = jnp.sum(stacked, axis=1, keepdims=True)
        line = jnp.sum(jnp.where(lane8 == row8, column, 0.0), axis=0, keepdims=True)
        dots[slot, me] = line

        def send(step, carry):
            target = device_of(lax.rem(me + step, devices))
            remote(
                dots.at[slot, me], dots.at[slot, me], dot_send.at[slot], dot_recv.at[slot], target
            ).start()
            return carry

        lax.fori_loop(1, devices, send, 0)

    def reduce_finish(slot, count):
        most = dots.at[slot, pl.ds(0, devices - 1)]
        pltpu.make_async_copy(most, most, dot_send.at[slot]).wait()
        pltpu.make_async_copy(most, most, dot_recv.at[slot]).wait()
        total = jnp.sum(dots[slot], axis=0)
        spread = jnp.sum(jnp.where(lane8 == row8, total, 0.0), axis=1, keepdims=True)
        spread = spread * (1.0 / total_count)
        return [jnp.broadcast_to(spread[n : n + 1, :], TILE) for n in range(count)]

    def inner_block(q, u):
        x = xall[q, u]
        at = pl.ds(pl.multiple_of(q * own_rows + u * half, half), half)

        def one(k, carry):
            value = jnp.dot(x, joint[k, 0], preferred_element_type=jnp.float32)
            value = value + jnp.dot(x, joint[k, 1], preferred_element_type=jnp.float32)
            inner[k, at, :] = value.astype(jnp.bfloat16)
            return carry

        lax.fori_loop(0, local_levels, one, 0)

    def rows_times(block, u):
        at = pl.ds(pl.multiple_of(block * own_rows + u * half, half), half)
        total = None
        for k in range(local_levels):
            term = jnp.dot(left[k, at, :], inner[k], preferred_element_type=jnp.float32)
            total = term if total is None else total + term
        return total

    def rows_times_part(block, u, q):
        at = pl.ds(pl.multiple_of(block * own_rows + u * half, half), half)
        span = pl.ds(pl.multiple_of(q * own_rows, own_rows), own_rows)
        total = None
        for k in range(local_levels):
            term = jnp.dot(
                left[k, at, span], inner[k, span, :], preferred_element_type=jnp.float32
            )
            total = term if total is None else total + term
        return total

    def exchange(t):
        return remote(wsend.at[t], wrecv.at[t], w_send.at[t], w_recv.at[t], partner)

    def piece_rows(piece):
        return pl.ds(piece * (half // 2), half // 2)

    def scatter(t, piece):
        block = target_block(t)
        right = block > i
        towards = jnp.where(right, i + 1, i - 1)
        slot = jnp.where(block == i - 1, n_lb, block)
        at = piece_rows(piece)
        return remote(
            zsend.at[t, at], zrecv.at[slot, at], z_send.at[2 * t + piece],
            z_recv.at[2 * slot + piece], (towards, j, w),
        )

    def arrived(slot, piece):
        at = piece_rows(piece)
        return pltpu.make_async_copy(
            zrecv.at[slot, at], zrecv.at[slot, at], z_recv.at[2 * slot + piece]
        )

    by_parts = own_rows % LANES == 0
    units = 2 * (n_lb - 1)

    def iteration(it, carry):
        def loaded(t):
            @pl.when(it == 0)
            def _():
                load_block(t).wait()

        first_block = target_block(0)
        loaded(0)

        def first_parts(q, start):
            if not by_parts:
                return
            for u, dst in ((other, wsend.at[0]), (w, img)):
                value = rows_times_part(first_block, u, q)
                dst[...] = value if start else dst[...] + value

        inner_block(j, w)
        gather_wa(0).wait_recv()
        inner_block(j, other)
        first_parts(j, True)

        def arrive(step, c):
            q = rb_step(step, -1)
            gather_rb(step).wait_recv()
            gather_wa(step).start()
            inner_block(q, w)
            gather_wa(step).wait_recv()
            inner_block(q, other)
            first_parts(q, False)
            return c

        lax.fori_loop(1, n_rb, arrive, 0)
        if not by_parts:
            wsend[0] = rows_times(first_block, other)
            img[...] = rows_times(first_block, w)

        def send_pieces(t):
            @pl.when(jnp.logical_not(interior))
            def _():
                for piece in range(2):
                    at = piece_rows(piece)
                    zsend[t, at] = wrecv[t, at].astype(jnp.bfloat16)
                    scatter(t, piece).start()

        def forward_piece(t, piece):
            @pl.when(interior)
            def _():
                block = target_block(t)
                arrived(block, piece).wait()
                at = piece_rows(piece)
                total = wrecv[t, at] + zrecv[block, at].astype(jnp.float32)
                zsend[t, at] = total.astype(jnp.bfloat16)
                scatter(t, piece).start()

        def forwards(unit):
            for t in range(n_lb - 1):
                if unit == min(2 * t + 2, units - 1):
                    forward_piece(t, 0)
                if unit == min(2 * t + 3, units):
                    forward_piece(t, 1)

        exchange(0).start()
        exchange(0).wait_recv()
        wrecv[0] = wrecv[0] + img[...]
        send_pieces(0)
        for t in range(1, n_lb):
            block = target_block(t)
            loaded(t)
            wsend[t] = rows_times(block, other)
            exchange(t).start()
            forwards(2 * t - 1)
            value = rows_times(block, w)
            exchange(t).wait_recv()
            if t < n_lb - 1:
                wrecv[t] = value + wrecv[t]
                send_pieces(t)
            else:
                img[...] = value + wrecv[t]
            forwards(2 * t)

        @pl.when(it == 0)
        def _():
            def mine(c, carry):
                diag[rows_at(c * chunk), :] = diagonal_part(w * half + c * chunk)
                return carry

            def theirs(c, carry):
                images[ITERS, rows_at(c * chunk), :] = diagonal_part(other * half + c * chunk)
                return carry

            over_chunks(theirs, 0)
            swap = remote(images.at[ITERS], basis.at[ITERS], d_sem.at[0], d_sem.at[1], partner)
            swap.start()
            over_chunks(mine, 0)
            swap.wait()

            def join(c, carry):
                at = rows_at(c * chunk)
                diag[at, :] = diag[at, :] + basis[ITERS, at, :]
                return carry

            over_chunks(join, 0)

        gather_wa(0).wait_send()
        for step in range(1, n_rb):
            gather_rb(step).wait_send()
            gather_wa(step).wait_send()
        for t in range(n_lb):
            exchange(t).wait_send()
        for t in range(n_lb - 1):
            for piece in range(2):
                scatter(t, piece).wait_send()

        @pl.when(it > 0)
        def _():
            for n, value in enumerate(reduce_finish(0, ITERS)):
                over[n] = value

        @pl.when(i > 0)
        def _():
            for piece in range(2):
                arrived(i, piece).wait()

        @pl.when(i < n_lb - 1)
        def _():
            for piece in range(2):
                arrived(n_lb, piece).wait()

        def measure(c, sums):
            at = rows_at(c * chunk)
            y = img[at, :] + (
                zrecv[i, at, :].astype(jnp.float32) + zrecv[n_lb, at, :].astype(jnp.float32)
            )
            x = vec[at, :]
            members = [basis[n, at, :] for n in range(ITERS)]
            for n in range(ITERS):
                overlap = scalar_of(over[n])
                x = x - overlap * members[n]
                y = y - overlap * images[n, at, :]
            vec[at, :] = x
            img[at, :] = y
            parts = [x * x, x * y] + [member * y for member in members]
            return tuple(total + fold(part) for total, part in zip(sums, parts))

        zero = jnp.zeros(TILE, jnp.float32)
        reduce_start(1, over_chunks(measure, (zero,) * (2 + ITERS)))
        sums = reduce_finish(1, 2 + ITERS)
        scale = lax.rsqrt(sums[0] + epsilon)

        def keep(c, carry):
            at = rows_at(c * chunk)
            basis[it, at, :] = vec[at, :] * scalar_of(scale)
            images[it, at, :] = img[at, :] * scalar_of(scale)
            return carry

        over_chunks(keep, 0)

        for order in range(1, ITERS + 2):

            @pl.when(it == order - 1)
            def _():
                last = order - 1
                for n in range(last):
                    sub[n * (ITERS + 1) + last] = sums[2 + n] * scale
                sub[last * (ITERS + 1) + last] = sums[1] * scale * scale
                value, weights = lowest_pair(order, lambda a, b: sub[a * (ITERS + 1) + b])
                pair[0] = value
                for n in range(ITERS + 1):
                    pair[n + 1] = weights[n] if n < order else zero

        def ritz(at, members):
            value = scalar_of(pair[0])
            weight = [scalar_of(pair[n + 1]) for n in range(members)]
            u = weight[0] * basis[0, at, :]
            r = weight[0] * images[0, at, :]
            for n in range(1, members):
                u = u + weight[n] * basis[n, at, :]
                r = r + weight[n] * images[n, at, :]
            return value, u, r - value * u

        @pl.when(it < ITERS)
        def _():
            def correct(c, sums):
                at = rows_at(c * chunk)
                value, _, r = ritz(at, ITERS)
                x = r / (jnp.abs(diag[at, :] - value) + 1.0)
                vec[at, :] = x
                xall[j, w, at, :] = x.astype(jnp.bfloat16)
                return tuple(
                    total + fold(basis[n, at, :] * x) for n, total in enumerate(sums)
                )

            overlaps = over_chunks(correct, (zero,) * ITERS)
            send_vector()
            reduce_start(0, overlaps)

        @pl.when(it == ITERS)
        def _():
            def finish(c, carry):
                at = rows_at(c * chunk)
                _, u, r = ritz(at, ITERS + 1)
                vec[at, :] = u
                img[at, :] = r
                return carry

            over_chunks(finish, 0)
            span = pl.ds(pl.multiple_of(w * half, half), half)
            moves = []
            for n, (src, dst) in enumerate(((vec, vec_out), (img, res_out))):
                moves.append(
                    remote(src, dst.at[span, :], out_sem.at[3 * n], out_sem.at[3 * n + 1], partner)
                )
                moves.append(pltpu.make_async_copy(src, dst.at[span, :], out_sem.at[3 * n + 2]))
            for move in moves:
                move.start()
            for move in moves:
                move.wait()

        return carry

    lax.fori_loop(0, ITERS + 1, iteration, 0)


def minor_of(size):
    best = 1
    for candidate in range(1, size + 1):
        if candidate * candidate <= size and size % candidate == 0:
            best = candidate
    return best


def per_device(initial_guess, left_environment, right_environment, operator_blocks, operator_pairs):
    own_rows, physical, window = initial_guess.shape
    width = physical * window
    levels = right_environment.shape[1]
    local_levels, coarse = left_environment.shape[:2]
    contracted = left_environment.shape[4]
    n_lb, n_rb, n_wa = lax.axis_size("lb"), lax.axis_size("rb"), lax.axis_size("wa")
    half = own_rows // n_wa
    total_count = own_rows * physical * window * n_lb * n_rb
    devices = n_lb * n_rb * n_wa

    operator = dense_operator(operator_blocks, operator_pairs, levels).reshape(-1)
    right = jnp.transpose(right_environment, (1, 0, 2)).astype(jnp.float32)
    left_matrix = left_environment.reshape(local_levels, coarse * own_rows, contracted)
    guess = lax.dynamic_slice_in_dim(initial_guess, lax.axis_index("wa") * half, half, 0)
    guess = guess.reshape(half, width)

    dims = (n_lb, n_rb, n_wa, minor_of(n_rb), own_rows, half, width, window, physical, levels,
            local_levels, total_count)
    f32, bf16 = jnp.float32, jnp.bfloat16
    members = ITERS + 1
    dma = pltpu.SemaphoreType.DMA
    outs = jax.ShapeDtypeStruct((own_rows, width), f32)
    vmem = pl.BlockSpec(memory_space=pltpu.VMEM)
    hbm = pl.BlockSpec(memory_space=pl.ANY)
    vectors, residuals = pl.pallas_call(
        functools.partial(davidson_kernel, dims),
        out_shape=(outs, outs),
        in_specs=[pl.BlockSpec(memory_space=pltpu.SMEM), vmem, vmem, hbm],
        out_specs=(hbm, hbm),
        scratch_shapes=[
            pltpu.VMEM((local_levels, coarse * own_rows, contracted), bf16),
            pltpu.VMEM((local_levels, 2, width, width), bf16),
            pltpu.VMEM((n_rb, n_wa, half, width), bf16),
            pltpu.VMEM((local_levels, contracted, width), bf16),
            pltpu.VMEM((n_lb, half, width), f32),
            pltpu.VMEM((n_lb, half, width), f32),
            pltpu.VMEM((n_lb - 1, half, width), bf16),
            pltpu.VMEM((n_lb + 1, half, width), bf16),
            pltpu.VMEM((members, half, width), f32),
            pltpu.VMEM((members, half, width), f32),
            pltpu.VMEM((half, width), f32),
            pltpu.VMEM((half, width), f32),
            pltpu.VMEM((half, width), f32),
            pltpu.VMEM((local_levels, 1, width), f32),
            pltpu.VMEM((2, devices, 1, LANES), f32),
            pltpu.VMEM((members * members,) + TILE, f32),
            pltpu.VMEM((members + 1,) + TILE, f32),
            pltpu.VMEM((ITERS,) + TILE, f32),
            dma((n_lb,)),
            dma((n_rb,)),
            dma((n_rb,)),
            dma((n_rb,)),
            dma((n_rb,)),
            dma((n_lb,)),
            dma((n_lb,)),
            dma((2 * n_lb,)),
            dma((2 * n_lb + 2,)),
            dma((2,)),
            dma((2,)),
            dma((2,)),
            dma((6,)),
        ],
        compiler_params=pltpu.CompilerParams(
            collective_id=0, has_side_effects=True, vmem_limit_bytes=VMEM_BYTES
        ),
        name="davidson",
    )(operator, guess, right, left_matrix)

    shape = (own_rows, physical, window)
    return vectors.reshape(shape), residuals.reshape(shape)


def solution(mesh):
    in_specs = (P(("lb", "rb"), None, None), P("wa", None, "rb", None, "lb"), P(), P(), P())
    out_specs = (P(("lb", "rb"), None, None), P(("lb", "rb"), None, None))
    return jax.shard_map(
        per_device, mesh=mesh, in_specs=in_specs, out_specs=out_specs, check_vma=False
    )
```

```python
import functools

import jax
import jax.numpy as jnp
from jax import lax
from jax.experimental import pallas as pl
from jax.experimental.pallas import tpu as pltpu
from jax.sharding import PartitionSpec as P

ITERS = 3
SWEEPS = 8

highest = lax.Precision.HIGHEST
epsilon = 1e-06

TILE = (8, 128)
LANES = 128
VMEM_BYTES = 66_000_000
MESH_IDS = pl.DeviceIdType.MESH


def half_angle(y, x):
    scale = jnp.maximum(jnp.abs(x), jnp.abs(y))
    zero = scale == 0.0
    inverse = 1.0 / jnp.where(zero, 1.0, scale)
    xs, ys = x * inverse, y * inverse
    h = jnp.sqrt(xs * xs + ys * ys)
    h = jnp.where(zero, 1.0, h)
    big = jnp.sqrt(0.5 * (1.0 + jnp.abs(xs) / h))
    small = 0.5 * jnp.abs(ys) / (h * big)
    positive = x >= 0.0
    cosine = jnp.where(positive, big, small)
    sine = jnp.where(positive, small, big) * jnp.where(y < 0.0, -1.0, 1.0)
    return jnp.where(zero, 1.0, cosine), jnp.where(zero, 0.0, sine)


def lowest_pair(order, entry):
    def at(i, j):
        return (min(i, j), max(i, j))

    one, none = jnp.full(TILE, 1.0, jnp.float32), jnp.full(TILE, 0.0, jnp.float32)
    if order == 1:
        return entry(0, 0), [one]
    keys = [(i, j) for i in range(order) for j in range(i, order)]
    start = tuple(entry(i, j) for i, j in keys)
    vectors0 = tuple(one if i == j else none for i in range(order) for j in range(order))

    def sweep(_, carry):
        m = dict(zip(keys, carry[0]))
        v = list(carry[1])
        for p in range(order):
            for q in range(p + 1, order):
                a, b, d = m[(p, p)], m[(p, q)], m[(q, q)]
                c, s = half_angle(2.0 * b, d - a)
                m[(p, p)] = c * (c * a - s * b) - s * (c * b - s * d)
                m[(p, q)] = s * (c * a - s * b) + c * (c * b - s * d)
                m[(q, q)] = s * (s * a + c * b) + c * (s * b + c * d)
                for i in range(order):
                    if i != p and i != q:
                        x, y = m[at(i, p)], m[at(i, q)]
                        m[at(i, p)] = c * x - s * y
                        m[at(i, q)] = s * x + c * y
                    x, y = v[i * order + p], v[i * order + q]
                    v[i * order + p] = c * x - s * y
                    v[i * order + q] = s * x + c * y
        return tuple(m[key] for key in keys), tuple(v)

    values, vectors = lax.fori_loop(0, SWEEPS, sweep, (start, vectors0))
    m = dict(zip(keys, values))
    best = m[(0, 0)]
    weights = [vectors[i * order] for i in range(order)]
    for j in range(1, order):
        better = m[(j, j)] < best
        best = jnp.where(better, m[(j, j)], best)
        weights = [
            jnp.where(better, vectors[i * order + j], weights[i]) for i in range(order)
        ]
    sign = jnp.where(weights[0] < 0.0, -1.0, 1.0)
    return best, [weight * sign for weight in weights]


def dense_operator(operator_blocks, operator_pairs, levels):
    blocks, physical, _ = operator_blocks.shape
    square = physical * physical
    symmetric = 0.5 * (operator_blocks + jnp.swapaxes(operator_blocks, 1, 2))
    entries = symmetric.reshape(blocks, 1, square)
    place = lax.broadcasted_iota(jnp.int32, (1, levels * levels, 1), 1)
    wanted = operator_pairs[:, 0] * levels + operator_pairs[:, 1]
    return jnp.sum(jnp.where(place == wanted[:, None, None], entries, 0.0), axis=0)


def fold(block):
    rows, columns = block.shape
    total = None
    for r in range(0, rows, TILE[0]):
        for c in range(0, columns, LANES):
            piece = block[r : r + TILE[0], c : c + LANES]
            total = piece if total is None else total + piece
    return total


def scalar_of(tile):
    return tile[0:1, 0:1]


def davidson_kernel(
    dims,
    op_ref, guess_ref, right_ref, left_hbm,
    vec_out, res_out,
    left, joint, xall, inner, wsend, wrecv, zsend, zrecv,
    basis, images, diag, vec, img, rows_ref, dots, sub, pair, over, sizes, right_f32, out3,
    load_sem, gx_send, gx_recv, gw_send, gw_recv, w_send, w_recv, z_send, z_recv,
    d_sem, dot_send, dot_recv, out_sem,
):
    (n_lb, n_rb, n_wa, rb_minor, own_rows, half, width, window, physical, levels,
     local_levels, total_count) = dims
    devices = n_lb * n_rb * n_wa
    i, j, w = lax.axis_index("lb"), lax.axis_index("rb"), lax.axis_index("wa")
    me = (i * n_rb + j) * n_wa + w
    other = 1 - w
    partner = (i, j, other)
    chunk = min(32, half)
    rb_major = n_rb // rb_minor

    def device_of(flat):
        return (
            lax.div(flat, n_rb * n_wa),
            lax.rem(lax.div(flat, n_wa), n_rb),
            lax.rem(flat, n_wa),
        )

    def rb_step(step, sign):
        high, low = lax.div(j, rb_minor), lax.rem(j, rb_minor)
        dh, dl = lax.div(step, rb_minor), lax.rem(step, rb_minor)
        if sign > 0:
            high, low = lax.rem(high + dh, rb_major), lax.rem(low + dl, rb_minor)
        else:
            high = lax.rem(high - dh + rb_major, rb_major)
            low = lax.rem(low - dl + rb_minor, rb_minor)
        return high * rb_minor + low

    def remote(src, dst, send, recv, target):
        return pltpu.make_async_remote_copy(
            src_ref=src, dst_ref=dst, send_sem=send, recv_sem=recv,
            device_id=target, device_id_type=MESH_IDS,
        )

    def rows_at(index, size=chunk):
        return pl.ds(pl.multiple_of(index, size), size)

    def over_chunks(body, init):
        return lax.fori_loop(0, half // chunk, body, init)

    barrier = pltpu.get_barrier_semaphore()

    def greet(step, carry):
        target = device_of(lax.rem(me + step, devices))
        pl.semaphore_signal(barrier, inc=1, device_id=target, device_id_type=MESH_IDS)
        return carry

    lax.fori_loop(1, devices, greet, 0)

    long_side = jnp.maximum(i, n_lb - 1 - i)
    short_side = jnp.minimum(i, n_lb - 1 - i)
    toward = jnp.where(2 * i <= n_lb - 1, 1, -1)
    interior = jnp.logical_and(i > 0, i < n_lb - 1)

    def target_block(t):
        if t == n_lb - 1:
            return i
        rest = t - (long_side - short_side)
        pair_at = jnp.maximum(rest, 0)
        near = short_side - lax.div(pair_at, 2)
        sign = jnp.where(lax.rem(pair_at, 2) == 0, -toward, toward)
        return jnp.where(rest < 0, i + toward * (long_side - t), i + sign * near)

    def load_block(t):
        span = pl.ds(pl.multiple_of(target_block(t) * own_rows, own_rows), own_rows)
        return pltpu.make_async_copy(
            left_hbm.at[:, span, :], left.at[:, span, :], load_sem.at[t]
        )

    for t in range(n_lb):
        load_block(t).start()

    xall[j, w] = guess_ref[...]

    def prepare(c, carry):
        at = rows_at(c * chunk)
        vec[at, :] = guess_ref[at, :].astype(jnp.float32)
        zeros = jnp.zeros((chunk, width), jnp.float32)
        for n in range(ITERS):
            basis[n, at, :] = zeros
            images[n, at, :] = zeros
        return carry

    over_chunks(prepare, 0)
    for n in range(ITERS):
        over[n] = jnp.zeros(TILE, jnp.float32)
    for n in range(ITERS + 1):
        sizes[n] = jnp.zeros(TILE, jnp.float32)

    @pl.when(i == 0)
    def _():
        zrecv[i] = jnp.zeros((half, width), jnp.bfloat16)

    @pl.when(i == n_lb - 1)
    def _():
        zrecv[n_lb] = jnp.zeros((half, width), jnp.bfloat16)

    pl.semaphore_wait(barrier, devices - 1)

    relayed = rb_major == 2 and rb_minor == 2
    direct = range(1, 3) if relayed else range(1, n_rb)
    quarter = half // 2

    def piece_rows(piece):
        return pl.ds(piece * quarter, quarter)

    def gather_rb(step, piece):
        q, at = rb_step(step, 1), piece_rows(piece)
        return remote(
            xall.at[j, w, at], xall.at[j, w, at], gx_send.at[2 * step + piece],
            gx_recv.at[2 * step + piece], (i, q, w),
        )

    def relay(piece):
        source, onward = rb_step(2 - w, -1), rb_step(1 + w, 1)
        at = piece_rows(piece)
        return remote(
            xall.at[source, w, at], xall.at[source, w, at], gx_send.at[6 + piece],
            gx_recv.at[6 + piece], (i, onward, w),
        )

    def gathered(step, piece):
        mine = xall.at[rb_step(step, -1), w, piece_rows(piece)]
        return pltpu.make_async_copy(mine, mine, gx_recv.at[2 * step + piece])

    def gather_wa(step, piece):
        q, at = rb_step(step, -1), piece_rows(piece)
        return remote(
            xall.at[q, w, at], xall.at[q, w, at], gw_send.at[2 * step + piece],
            gw_recv.at[2 * step + piece], partner,
        )

    def send_vector():
        for piece in range(2):
            for step in direct:
                gather_rb(step, piece).start()
            gather_wa(0, piece).start()

    send_vector()

    right_f32[...] = right_ref[...].astype(jnp.float32)

    op_base = w * (local_levels * levels)
    band = min(32, window)

    def make_joint(index, carry):
        k = lax.div(index, window // band)
        r0 = lax.rem(index, window // band) * band
        mats = [right_f32[pl.ds(pl.multiple_of(r0, band), band), v, :] for v in range(levels)]
        for s in range(physical):
            for t in range(physical):
                total = None
                for v in range(levels):
                    term = op_ref[op_base + k * levels + v, t * physical + s] * mats[v]
                    total = term if total is None else total + term
                high = total.astype(jnp.bfloat16)
                low = (total - high.astype(jnp.float32)).astype(jnp.bfloat16)
                rows = pl.ds(pl.multiple_of(s * window + r0, band), band)
                joint[k, 0, rows, t * window : (t + 1) * window] = high
                joint[k, 1, rows, t * window : (t + 1) * window] = low
        return carry

    lax.fori_loop(0, local_levels * (window // band), make_joint, 0)

    eye = lax.broadcasted_iota(jnp.int32, (window, window), 0) == lax.broadcasted_iota(
        jnp.int32, (window, window), 1
    )
    right_diag = [
        jnp.sum(jnp.where(eye, right_f32[:, v, :], 0.0), axis=0, keepdims=True) for v in range(levels)
    ]
    for k in range(local_levels):
        for s in range(physical):
            total = None
            for v in range(levels):
                term = op_ref[op_base + k * levels + v, s * physical + s] * right_diag[v]
                total = term if total is None else total + term
            rows_ref[k, :, s * window : (s + 1) * window] = total

    def diagonal_part(r0):
        first = j * own_rows + r0
        base = lax.div(first, LANES) * LANES
        shift = first - base
        lane = lax.broadcasted_iota(jnp.int32, (chunk, LANES), 1)
        row = lax.broadcasted_iota(jnp.int32, (chunk, LANES), 0)
        mask = lane == row + shift
        total = None
        for k in range(local_levels):
            block = left[
                k,
                pl.ds(pl.multiple_of(i * own_rows + r0, chunk), chunk),
                pl.ds(pl.multiple_of(base, LANES), LANES),
            ].astype(jnp.float32)
            column = jnp.sum(jnp.where(mask, block, 0.0), axis=1, keepdims=True)
            term = column * rows_ref[k]
            total = term if total is None else total + term
        return total

    lane8 = lax.broadcasted_iota(jnp.int32, TILE, 1)
    row8 = lax.broadcasted_iota(jnp.int32, TILE, 0)

    def reduce_start(slot, tiles):
        rows = [jnp.sum(tile, axis=0, keepdims=True) for tile in tiles]
        stacked = jnp.zeros(TILE, jnp.float32)
        for n, row in enumerate(rows):
            stacked = jnp.where(row8 == n, row, stacked)
        column = jnp.sum(stacked, axis=1, keepdims=True)
        line = jnp.sum(jnp.where(lane8 == row8, column, 0.0), axis=0, keepdims=True)
        dots[slot, me] = line

        def send(step, carry):
            target = device_of(lax.rem(me + step, devices))
            remote(
                dots.at[slot, me], dots.at[slot, me], dot_send.at[slot], dot_recv.at[slot], target
            ).start()
            return carry

        lax.fori_loop(1, devices, send, 0)

    def reduce_finish(slot, count):
        most = dots.at[slot, pl.ds(0, devices - 1)]
        pltpu.make_async_copy(most, most, dot_send.at[slot]).wait()
        pltpu.make_async_copy(most, most, dot_recv.at[slot]).wait()
        total = jnp.sum(dots[slot], axis=0)
        spread = jnp.sum(jnp.where(lane8 == row8, total, 0.0), axis=1, keepdims=True)
        spread = spread * (1.0 / total_count)
        return [jnp.broadcast_to(spread[n : n + 1, :], TILE) for n in range(count)]

    def inner_block(q, u):
        x = xall[q, u]
        at = pl.ds(pl.multiple_of(q * own_rows + u * half, half), half)

        def one(k, carry):
            value = jnp.dot(x, joint[k, 0], preferred_element_type=jnp.float32)
            value = value + jnp.dot(x, joint[k, 1], preferred_element_type=jnp.float32)
            inner[k, at, :] = value.astype(jnp.bfloat16)
            return carry

        lax.fori_loop(0, local_levels, one, 0)

    def inner_pieces(blocks, u, piece):
        x = jnp.concatenate([xall[q, u, piece_rows(piece)] for q in blocks], axis=0)

        def one(k, carry):
            value = jnp.dot(x, joint[k, 0], preferred_element_type=jnp.float32)
            value = value + jnp.dot(x, joint[k, 1], preferred_element_type=jnp.float32)
            value = value.astype(jnp.bfloat16)
            for n, q in enumerate(blocks):
                first = q * own_rows + u * half + piece * quarter
                at = pl.ds(pl.multiple_of(first, quarter), quarter)
                inner[k, at, :] = value[n * quarter : (n + 1) * quarter]
            return carry

        lax.fori_loop(0, local_levels, one, 0)

    def rows_times(block, u):
        at = pl.ds(pl.multiple_of(block * own_rows + u * half, half), half)
        total = None
        for k in range(local_levels):
            term = jnp.dot(left[k, at, :], inner[k], preferred_element_type=jnp.float32)
            total = term if total is None else total + term
        return total

    def rows_times_part(block, u, q):
        at = pl.ds(pl.multiple_of(block * own_rows + u * half, half), half)
        span = pl.ds(pl.multiple_of(q * own_rows, own_rows), own_rows)
        total = None
        for k in range(local_levels):
            term = jnp.dot(
                left[k, at, span], inner[k, span, :], preferred_element_type=jnp.float32
            )
            total = term if total is None else total + term
        return total

    def exchange(t):
        return remote(wsend.at[t], wrecv.at[t], w_send.at[t], w_recv.at[t], partner)

    def scatter(t, piece):
        block = target_block(t)
        right = block > i
        towards = jnp.where(right, i + 1, i - 1)
        slot = jnp.where(block == i - 1, n_lb, block)
        at = piece_rows(piece)
        return remote(
            zsend.at[t, at], zrecv.at[slot, at], z_send.at[2 * t + piece],
            z_recv.at[2 * slot + piece], (towards, j, w),
        )

    def arrived(slot, piece):
        at = piece_rows(piece)
        return pltpu.make_async_copy(
            zrecv.at[slot, at], zrecv.at[slot, at], z_recv.at[2 * slot + piece]
        )

    by_parts = own_rows % LANES == 0
    units = 2 * (n_lb - 1)

    def iteration(it, carry):
        def loaded(t):
            @pl.when(it == 0)
            def _():
                load_block(t).wait()

        first_block = target_block(0)
        loaded(0)

        def first_parts(q, start, last):
            if not by_parts:
                return
            for u, dst in ((other, wsend.at[0]), (w, img)):
                value = rows_times_part(first_block, u, q)
                dst[...] = value if start else dst[...] + value
                if u is other and last is not False:

                    @pl.when(last)
                    def _():
                        exchange(0).start()

        inner_block(j, w)
        for piece in range(2):
            gather_wa(0, piece).wait_recv()
        inner_block(j, other)
        first_parts(j, True, n_rb == 1)

        def arrive(step, c):
            q = rb_step(step, -1)
            for piece in range(2):
                gathered(step, piece).wait()
                gather_wa(step, piece).start()
            inner_block(q, w)
            for piece in range(2):
                gather_wa(step, piece).wait_recv()
            inner_block(q, other)
            first_parts(q, False, step == n_rb - 1)
            return c

        if relayed:
            near = [rb_step(1, -1), rb_step(2, -1)]
            far = rb_step(3, -1)
            for piece in range(2):
                for step in direct:
                    gathered(step, piece).wait()
                relay(piece).start()
                for step in direct:
                    gather_wa(step, piece).start()
                inner_pieces(near, w, piece)
                for step in direct:
                    gather_wa(step, piece).wait_recv()
                inner_pieces(near, other, piece)
            for piece in range(2):
                first_parts(near[piece], False, False)
                gathered(3, piece).wait()
                gather_wa(3, piece).start()
            inner_block(far, w)
            for piece in range(2):
                gather_wa(3, piece).wait_recv()
            inner_block(far, other)
            first_parts(far, False, True)
        else:
            lax.fori_loop(1, n_rb, arrive, 0)
        if not by_parts:
            wsend[0] = rows_times(first_block, other)
            exchange(0).start()
            img[...] = rows_times(first_block, w)

        def send_pieces(t):
            @pl.when(jnp.logical_not(interior))
            def _():
                for piece in range(2):
                    at = piece_rows(piece)
                    zsend[t, at] = wrecv[t, at].astype(jnp.bfloat16)
                    scatter(t, piece).start()

        def forward_piece(t, piece):
            @pl.when(interior)
            def _():
                block = target_block(t)
                arrived(block, piece).wait()
                at = piece_rows(piece)
                total = wrecv[t, at] + zrecv[block, at].astype(jnp.float32)
                zsend[t, at] = total.astype(jnp.bfloat16)
                scatter(t, piece).start()

        def forwards(unit):
            for t in range(n_lb - 1):
                if unit == min(2 * t + 2, units - 1):
                    forward_piece(t, 0)
                if unit == min(2 * t + 3, units):
                    forward_piece(t, 1)

        exchange(0).wait_recv()
        wrecv[0] = wrecv[0] + img[...]
        send_pieces(0)
        for t in range(1, n_lb):
            block = target_block(t)
            loaded(t)
            wsend[t] = rows_times(block, other)
            exchange(t).start()
            forwards(2 * t - 1)
            value = rows_times(block, w)
            exchange(t).wait_recv()
            if t < n_lb - 1:
                wrecv[t] = value + wrecv[t]
                send_pieces(t)
            else:
                img[...] = value + wrecv[t]
            forwards(2 * t)

        @pl.when(it == 0)
        def _():
            def mine(c, carry):
                diag[rows_at(c * chunk), :] = diagonal_part(w * half + c * chunk)
                return carry

            def theirs(c, carry):
                images[ITERS, rows_at(c * chunk), :] = diagonal_part(other * half + c * chunk)
                return carry

            over_chunks(theirs, 0)
            swap = remote(images.at[ITERS], basis.at[ITERS], d_sem.at[0], d_sem.at[1], partner)
            swap.start()
            over_chunks(mine, 0)
            swap.wait()

            def join(c, carry):
                at = rows_at(c * chunk)
                diag[at, :] = diag[at, :] + basis[ITERS, at, :]
                return carry

            over_chunks(join, 0)

        for piece in range(2):
            for step in direct:
                gather_rb(step, piece).wait_send()
            for step in range(n_rb):
                gather_wa(step, piece).wait_send()
            if relayed:
                relay(piece).wait_send()
        for t in range(n_lb):
            exchange(t).wait_send()
        for t in range(n_lb - 1):
            for piece in range(2):
                scatter(t, piece).wait_send()

        @pl.when(it > 0)
        def _():
            for n, value in enumerate(reduce_finish(0, ITERS)):
                over[n] = value * sizes[n] * sizes[n]

        @pl.when(i > 0)
        def _():
            for piece in range(2):
                arrived(i, piece).wait()

        @pl.when(i < n_lb - 1)
        def _():
            for piece in range(2):
                arrived(n_lb, piece).wait()

        def measure(c, sums):
            at = rows_at(c * chunk)
            y = img[at, :] + (
                zrecv[i, at, :].astype(jnp.float32) + zrecv[n_lb, at, :].astype(jnp.float32)
            )
            x = vec[at, :]
            members = [basis[n, at, :] for n in range(ITERS)]
            for n in range(ITERS):
                overlap = scalar_of(over[n])
                x = x - overlap * members[n]
                y = y - overlap * images[n, at, :]
            basis[it, at, :] = x
            images[it, at, :] = y
            parts = [x * x, x * y] + [member * y for member in members]
            return tuple(total + fold(part) for total, part in zip(sums, parts))

        zero = jnp.zeros(TILE, jnp.float32)
        reduce_start(1, over_chunks(measure, (zero,) * (2 + ITERS)))
        sums = reduce_finish(1, 2 + ITERS)
        scale = lax.rsqrt(sums[0] + epsilon)

        sizes[it] = scale

        for order in range(1, ITERS + 2):

            @pl.when(it == order - 1)
            def _():
                last = order - 1
                for n in range(last):
                    sub[n * (ITERS + 1) + last] = sums[2 + n] * sizes[n] * scale
                sub[last * (ITERS + 1) + last] = sums[1] * scale * scale
                value, weights = lowest_pair(order, lambda a, b: sub[a * (ITERS + 1) + b])
                pair[0] = value
                for n in range(ITERS + 1):
                    pair[n + 1] = weights[n] * sizes[n] if n < order else zero

        def ritz(at, members):
            value = scalar_of(pair[0])
            weight = [scalar_of(pair[n + 1]) for n in range(members)]
            u = weight[0] * basis[0, at, :]
            r = weight[0] * images[0, at, :]
            for n in range(1, members):
                u = u + weight[n] * basis[n, at, :]
                r = r + weight[n] * images[n, at, :]
            return value, u, r - value * u

        @pl.when(it < ITERS)
        def _():
            def correct(c, sums):
                at = rows_at(c * chunk)
                value, _, r = ritz(at, ITERS)
                x = r / (jnp.abs(diag[at, :] - value) + 1.0)
                vec[at, :] = x
                xall[j, w, at, :] = x.astype(jnp.bfloat16)
                return tuple(
                    total + fold(basis[n, at, :] * x) for n, total in enumerate(sums)
                )

            overlaps = over_chunks(correct, (zero,) * ITERS)
            send_vector()
            reduce_start(0, overlaps)

        @pl.when(it == ITERS)
        def _():
            def finish(c, carry):
                at = rows_at(c * chunk)
                _, u, r = ritz(at, ITERS + 1)
                for s in range(physical):
                    out3[0, at, s, :] = u[:, s * window : (s + 1) * window]
                    out3[1, at, s, :] = r[:, s * window : (s + 1) * window]
                return carry

            over_chunks(finish, 0)
            span = pl.ds(pl.multiple_of(w * half, half), half)
            moves = []
            for n, (src, dst) in enumerate(((out3.at[0], vec_out), (out3.at[1], res_out))):
                moves.append(
                    remote(src, dst.at[span], out_sem.at[3 * n], out_sem.at[3 * n + 1], partner)
                )
                moves.append(pltpu.make_async_copy(src, dst.at[span], out_sem.at[3 * n + 2]))
            for move in moves:
                move.start()
            for move in moves:
                move.wait()

        return carry

    lax.fori_loop(0, ITERS + 1, iteration, 0)


def minor_of(size):
    best = 1
    for candidate in range(1, size + 1):
        if candidate * candidate <= size and size % candidate == 0:
            best = candidate
    return best


def per_device(initial_guess, left_environment, right_environment, operator_blocks, operator_pairs):
    own_rows, physical, window = initial_guess.shape
    width = physical * window
    levels = right_environment.shape[1]
    local_levels, coarse = left_environment.shape[:2]
    contracted = left_environment.shape[4]
    n_lb, n_rb, n_wa = lax.axis_size("lb"), lax.axis_size("rb"), lax.axis_size("wa")
    half = own_rows // n_wa
    total_count = own_rows * physical * window * n_lb * n_rb
    devices = n_lb * n_rb * n_wa

    operator = dense_operator(operator_blocks, operator_pairs, levels)
    left_matrix = left_environment.reshape(local_levels, coarse * own_rows, contracted)
    guess = lax.dynamic_slice_in_dim(initial_guess, lax.axis_index("wa") * half, half, 0)
    guess = guess.reshape(half, width)

    dims = (n_lb, n_rb, n_wa, minor_of(n_rb), own_rows, half, width, window, physical, levels,
            local_levels, total_count)
    f32, bf16 = jnp.float32, jnp.bfloat16
    members = ITERS + 1
    dma = pltpu.SemaphoreType.DMA
    outs = jax.ShapeDtypeStruct((own_rows, physical, window), f32)
    vmem = pl.BlockSpec(memory_space=pltpu.VMEM)
    hbm = pl.BlockSpec(memory_space=pl.ANY)
    return pl.pallas_call(
        functools.partial(davidson_kernel, dims),
        out_shape=(outs, outs),
        in_specs=[pl.BlockSpec(memory_space=pltpu.SMEM), vmem, vmem, hbm],
        out_specs=(hbm, hbm),
        scratch_shapes=[
            pltpu.VMEM((local_levels, coarse * own_rows, contracted), bf16),
            pltpu.VMEM((local_levels, 2, width, width), bf16),
            pltpu.VMEM((n_rb, n_wa, half, width), bf16),
            pltpu.VMEM((local_levels, contracted, width), bf16),
            pltpu.VMEM((n_lb, half, width), f32),
            pltpu.VMEM((n_lb, half, width), f32),
            pltpu.VMEM((n_lb - 1, half, width), bf16),
            pltpu.VMEM((n_lb + 1, half, width), bf16),
            pltpu.VMEM((members, half, width), f32),
            pltpu.VMEM((members, half, width), f32),
            pltpu.VMEM((half, width), f32),
            pltpu.VMEM((half, width), f32),
            pltpu.VMEM((half, width), f32),
            pltpu.VMEM((local_levels, 1, width), f32),
            pltpu.VMEM((2, devices, 1, LANES), f32),
            pltpu.VMEM((members * members,) + TILE, f32),
            pltpu.VMEM((members + 1,) + TILE, f32),
            pltpu.VMEM((ITERS,) + TILE, f32),
            pltpu.VMEM((members,) + TILE, f32),
            pltpu.VMEM((window, levels, window), f32),
            pltpu.VMEM((2, half, physical, window), f32),
            dma((n_lb,)),
            dma((2 * n_rb,)),
            dma((2 * n_rb,)),
            dma((2 * n_rb,)),
            dma((2 * n_rb,)),
            dma((n_lb,)),
            dma((n_lb,)),
            dma((2 * n_lb,)),
            dma((2 * n_lb + 2,)),
            dma((2,)),
            dma((2,)),
            dma((2,)),
            dma((6,)),
        ],
        compiler_params=pltpu.CompilerParams(
            collective_id=0, has_side_effects=True, vmem_limit_bytes=VMEM_BYTES
        ),
        name="davidson",
    )(operator, guess, right_environment, left_matrix)


def solution(mesh):
    in_specs = (P(("lb", "rb"), None, None), P("wa", None, "rb", None, "lb"), P(), P(), P())
    out_specs = (P(("lb", "rb"), None, None), P(("lb", "rb"), None, None))
    return jax.shard_map(
        per_device, mesh=mesh, in_specs=in_specs, out_specs=out_specs, check_vma=False
    )
```
